256 devices in a mesh: seq: 64 (over z, y, core), head: 4 (over x).
Axes of the slice: x: 4, y: 4, z: 8, core: 2. Of those that a mesh axis runs over, the one named last changes fastest.
Arguments:
- inputs: bfloat16 [16384, 5120], P('seq', 'head'), may hold values from -6 to 6
- time_step: float32 [80, 16384], P('head', 'seq'), may hold values from 0.01 to 0.3
- decay_rate: float32 [80], P('head'), may hold values from 0.0001 to 1
- input_map: bfloat16 [16384, 128], P('seq'), may hold values from -6 to 6
- output_map: bfloat16 [16384, 128], P('seq'), may hold values from -0.59765625 to 0.59765625
- output_grad: bfloat16 [16384, 5120], P('seq', 'head'), may hold values from -3 to 3
- span_states: float32 [64, 80, 64, 128], P('seq', 'head'), may hold values from -6 to 6
- resets: int32 [64], P('seq'), may hold values from 0 to 4095
Outputs:
- grad_inputs: bfloat16 [16384, 5120], P('seq', 'head')
- grad_input_map: float32 [16384, 128], P('seq')
- grad_rate: float32 [80], P('head')
The draws below stay inside these ranges and needn't reach their ends.
Inputs may be any that keep to these rules, and one draw needn't show every extreme that they name: `resets`: A value p under 256 means that a document starts at position p of that span; a value of 256 or more means that none starts in it.
All inputs are finite; a program needn't handle non-finite values.
Results may differ from the reference program's by a relative error of at most 0.003.
Values sent between devices are 32-bit elements; how exact they have to be, the bound alone decides.
No kernel may reach another device: no remote copies, remote signals or barrier semaphores. Data moves between devices by JAX's collectives and lax.ppermute only.
A program may use at most 64 MiB of HBM per device.

```python
import math
import jax
import jax.numpy as jnp
from jax import lax

NHEADS = 80
HEADDIM = 64
DSTATE = 128
SPAN = 256
TOKENS = 16384
NCHUNK = 64


def place_ends(array, stream_key, low, top_value):
    longest = array.shape.index(max(array.shape))
    spots = []
    for shift in (0, 1):
        where = [jax.random.randint(jax.random.fold_in(stream_key, axis), (), 0, length) for axis, length in enumerate(array.shape)]
        where[longest] = (where[longest] + shift) % array.shape[longest]
        spots.append(tuple(where))
    return array.at[spots[0]].set(low).at[spots[1]].set(top_value)


def steps_of(rng, dims, split, low, largest):
    factor_of = 1.0
    for dim, parts in split:
        heights = jax.random.uniform(jax.random.fold_in(jax.random.fold_in(rng, 6), dim), (parts,), jnp.float32, low / len(split), largest / len(split))
        factor_of = factor_of * jnp.repeat(jnp.exp(heights), dims[dim] // parts).reshape((-1,) + (1,) * (len(dims) - 1 - dim))
    return factor_of


def scatter_about(rng, extent, scale, bound, split=(), held_as=jnp.bfloat16):
    level = steps_of(rng, extent, split, -0.22, 0.18) if split else 1.0
    result = jax.random.normal(rng, extent, jnp.float32) * scale * level
    return jnp.minimum(jnp.maximum(result, -bound), bound).astype(held_as)


def setup_inputs(seed: int = 0) -> dict:
    streams_of = jax.random.split(jax.random.key(seed), 9)
    return {
        "inputs": scatter_about(streams_of[0], (TOKENS, NHEADS * HEADDIM), 1.0, 6.0, ((0, 64), (1, 4))),
        "time_step": jnp.clip(jnp.exp(math.log(0.3) - 3.4011974 * jax.random.uniform(streams_of[1], (NHEADS, TOKENS), jnp.float32) ** steps_of(streams_of[1], (NHEADS, TOKENS), ((0, 4), (1, 64)), -0.2, 0.2)), 0.01, 0.3),
        "decay_rate": jnp.clip(jnp.exp(math.log(1.0) - 9.2103404 * jax.random.uniform(streams_of[2], (NHEADS,), jnp.float32) ** steps_of(streams_of[2], (NHEADS,), ((0, 4),), -0.2, 0.2)), 0.0001, 1.0),
        "input_map": scatter_about(streams_of[3], (TOKENS, DSTATE), 1.0, 6.0, ((0, 64),)),
        "output_map": scatter_about(streams_of[4], (TOKENS, DSTATE), 0.1, 0.59765625, ((0, 64),)),
        "output_grad": scatter_about(streams_of[5], (TOKENS, NHEADS * HEADDIM), 0.5, 3.0, ((0, 64), (1, 4))),
        "span_states": scatter_about(streams_of[6], (NCHUNK, NHEADS, HEADDIM, DSTATE), 1.0, 6.0, ((0, 64), (1, 4)), jnp.float32),
        "resets": place_ends(jax.random.randint(streams_of[7], (NCHUNK,), 0, 16 * SPAN), jax.random.fold_in(streams_of[7], 1), 0, (16 * SPAN) - 1).astype(jnp.int32),
    }


highest = lax.Precision.HIGHEST


def prepare(x_block, step_block, decay_rate, b_block, c_block, grad_block, start_state, reset_at):
    block_len = step_block.shape[1]
    positions = jnp.arange(block_len, dtype=jnp.int32)
    later_doc = positions >= reset_at
    no_reset = reset_at >= block_len
    elapsed = jnp.cumsum(step_block, axis=1)
    log_decay = -decay_rate[:, None] * elapsed
    joined = (later_doc[:, None] == later_doc[None, :]) & (positions[None, :] >= positions[:, None])
    log_gaps = log_decay[:, None, :] - log_decay[:, :, None]
    pair_weight = jnp.where(joined[None], jnp.exp(jnp.where(joined[None], log_gaps, 0.0)), 0.0)
    intersection = jnp.dot(b_block, c_block.T, preferred_element_type=jnp.float32)
    products = jnp.einsum("shp,uhp->hsu", x_block.astype(jnp.float32), grad_block.astype(jnp.float32))
    mixing = (pair_weight * intersection[None]).astype(jnp.bfloat16)
    pair_terms = pair_weight * products
    paired = pair_terms.astype(jnp.bfloat16)
    dx_inner = jnp.einsum("hsu,uhp->shp", mixing.astype(jnp.float32), grad_block.astype(jnp.float32))
    db_inner = jnp.einsum("hsu,un->hsn", paired.astype(jnp.float32), c_block.astype(jnp.float32))
    start_weight = jnp.where(later_doc[None], 0.0, jnp.exp(log_decay))
    end_weight = jnp.where((later_doc | no_reset)[None], jnp.exp(log_decay[:, -1:] - log_decay), 0.0)
    carry_gain = jnp.where(no_reset, jnp.exp(log_decay[:, -1]), 0.0)
    c_wide = c_block.astype(jnp.float32)
    grad_wide = grad_block.astype(jnp.float32)
    weighted_c = start_weight[:, :, None] * c_wide[None]
    boundary_grad = jnp.einsum("hun,uhp->hpn", weighted_c, grad_wide, precision=highest)
    state_read = jnp.einsum("uhp,hpn->hun", grad_wide, start_state, precision=highest)
    start_term = jnp.sum(state_read * c_wide[None], axis=2)
    inside_term = jnp.sum(pair_terms * intersection[None] * step_block[:, :, None] * (elapsed[:, None, :] - elapsed[:, :, None]), axis=(1, 2))
    entry_term = jnp.sum(start_weight * elapsed * start_term, axis=1)
    return carry_gain, boundary_grad, dx_inner, db_inner, inside_term + entry_term, end_weight, elapsed


def finish(prepared, x_block, step_block, b_block, start_state, carried):
    carry_gain, boundary_grad, dx_inner, db_inner, partial_rate, end_weight, elapsed = prepared
    b_wide = b_block.astype(jnp.float32)
    x_wide = x_block.astype(jnp.float32)
    carried_b = jnp.einsum("sn,hpn->shp", b_wide, carried, precision=highest)
    carried_x = jnp.einsum("shp,hpn->hsn", x_wide, carried, precision=highest)
    step_rows = step_block.T[:, :, None]
    end_rows = end_weight.T[:, :, None]
    grad_x = (step_rows * (dx_inner + end_rows * carried_b)).astype(jnp.bfloat16)
    grad_b = jnp.sum(step_block[:, :, None] * (db_inner + end_weight[:, :, None] * carried_x), axis=0)
    last_elapsed = elapsed[:, -1]
    leaving_term = jnp.sum(end_weight * step_block * (last_elapsed[:, None] - elapsed) * jnp.sum(carried_x * b_wide[None], axis=2), axis=1)
    through_term = carry_gain * last_elapsed * jnp.sum(carried * start_state, axis=(1, 2))
    return grad_x, grad_b, partial_rate + leaving_term + through_term


def reference(inputs, time_step, decay_rate, input_map, output_map, output_grad, span_states, resets):
    x_all = inputs.reshape(NCHUNK, SPAN, NHEADS, HEADDIM)
    grad_all = output_grad.reshape(NCHUNK, SPAN, NHEADS, HEADDIM)
    step_all = time_step.reshape(NHEADS, NCHUNK, SPAN).transpose(1, 0, 2)
    b_all = input_map.reshape(NCHUNK, SPAN, DSTATE)
    c_all = output_map.reshape(NCHUNK, SPAN, DSTATE)

    def backward_block(carried, block_items):
        x_block, step_block, b_block, c_block, grad_block, start_state, reset_at = block_items
        prepared = prepare(x_block, step_block, decay_rate, b_block, c_block, grad_block, start_state, reset_at)
        grad_x, grad_b, rate_part = finish(prepared, x_block, step_block, b_block, start_state, carried)
        updated = prepared[1] + prepared[0][:, None, None] * carried
        return updated, (grad_x, grad_b, rate_part)

    initial = jnp.zeros((NHEADS, HEADDIM, DSTATE), jnp.float32)
    ending, outputs = lax.scan(backward_block, initial, (x_all, step_all, b_all, c_all, grad_all, span_states, resets.astype(jnp.int32)), reverse=True)
    grad_x_all, grad_b_all, rate_parts = outputs
    return (grad_x_all.reshape(TOKENS, NHEADS * HEADDIM), grad_b_all.reshape(TOKENS, DSTATE), -jnp.sum(rate_parts, axis=0))
```

```python
import functools

import jax
import jax.numpy as jnp
from jax import lax
from jax.experimental import pallas as pl
from jax.experimental.pallas import tpu as pltpu
from jax.sharding import Mesh
from jax.sharding import PartitionSpec as P

CHIPS = ("seq_0", "seq_1")
CORE = "seq_2"
SEQ = CHIPS + (CORE,)
f32, bf16 = jnp.float32, jnp.bfloat16

HEADS, WIDTH, STATE, SPAN = 20, 64, 128, 256
COLS = HEADS * WIDTH
HALF = COLS // 2
CHUNK = 256
STEPS = COLS // CHUNK
SHARES = 32
MIDDLE = SPAN // 2 - 1

NN = (((1,), (0,)), ((), ()))
NT = (((1,), (1,)), ((), ()))
TN = (((0,), (0,)), ((), ()))


def dot(a, b, dims):
    return lax.dot_general(a, b, dims, preferred_element_type=f32)


def two_parts(a):
    high = a.astype(bf16)
    return high, (a - high.astype(f32)).astype(bf16)


def three_parts(a):
    high = a.astype(bf16)
    rest = a - high.astype(f32)
    mid = rest.astype(bf16)
    return high, mid, (rest - mid.astype(f32)).astype(bf16)


def dot3(a, b, dims):
    return dot(a[0], b[0], dims) + (dot(a[0], b[1], dims) + dot(a[1], b[0], dims))


def iota(shape, dim):
    return lax.broadcasted_iota(jnp.int32, shape, dim)


def spread(chunk):
    shape = (128, CHUNK)
    lane = iota(shape, 0)
    head = (iota(shape, 1) + chunk * CHUNK) >> 6
    return jnp.where(((lane & 31) == head) & (lane < 96), 1.0, 0.0).astype(bf16)


def packed(a):
    high, mid, low = three_parts(a)
    lane = iota(a.shape, 1)
    return jnp.where(
        lane < 32, high.astype(f32), jnp.where(lane < 64, mid.astype(f32), low.astype(f32))
    ).astype(bf16)


def small_factors(rate_ref, step_ref, pad_ref, with_steps):
    pad_ref[...] = jnp.zeros_like(pad_ref)
    for copy in range(3):
        pad_ref[32 * copy : 32 * copy + HEADS, :] = step_ref[...]
    parts = three_parts(pad_ref[...])
    row, col = iota((SPAN, SPAN), 0), iota((SPAN, SPAN), 1)
    lower = jnp.where(col <= row, 1.0, 0.0).astype(bf16)
    elapsed = dot(lower, parts[0], NT) + (dot(lower, parts[1], NT) + dot(lower, parts[2], NT))
    lane = iota((1, 128), 1) & 31
    rate = jnp.zeros((1, 128), f32)
    for h in range(HEADS):
        rate = jnp.where(lane == h, rate_ref[h], rate)
    log_decay = -rate * elapsed
    if not with_steps:
        return elapsed, log_decay, None
    same = jnp.where(col == row, 1.0, 0.0).astype(bf16)
    steps = (dot(same, parts[0], NT) + dot(same, parts[1], NT)) + dot(same, parts[2], NT)
    return elapsed, log_decay, steps


def boundary_kernel(
    reset_ref, core_ref, rate_ref, step_ref, c_ref, grad_ref, keep_ref, send_ref, pad_ref, all_ref
):
    reset, core = reset_ref[0], core_ref[0]
    elapsed, log_decay, _ = small_factors(rate_ref, step_ref, pad_ref, False)
    later = iota((SPAN, 128), 0) >= reset
    weight = packed(jnp.where(later, 0.0, jnp.exp(log_decay)))
    gain = jnp.where(reset >= SPAN, jnp.exp(log_decay[SPAN - 1 :, :]), 0.0)
    gain = packed(jnp.broadcast_to(gain, (8, 128)))
    for chunk in range(STEPS):
        cols = pl.ds(chunk * CHUNK, CHUNK)
        wide = spread(chunk)
        weighted = dot(weight, wide, NN) * grad_ref[:, cols].astype(f32)
        high, low = two_parts(weighted)
        all_ref[:STATE, cols] = dot(c_ref[...], high, TN) + dot(c_ref[...], low, TN)
        all_ref[STATE:, cols] = dot(gain, wide, NN)
    keep_ref[...] = all_ref[:, pl.ds(pl.multiple_of(core * HALF, HALF), HALF)]
    send_ref[...] = all_ref[:, pl.ds(pl.multiple_of((1 - core) * HALF, HALF), HALF)]


def combine_kernel(core_ref, keep_ref, got_ref, out_ref):
    first = core_ref[0] == 0
    upper = iota((STATE, 128), 0) & 7

    def tile(t):
        cols = slice(128 * t, 128 * t + 128)
        keep, got = keep_ref[:, cols], got_ref[:, cols]
        early, late = jnp.where(first, keep, got), jnp.where(first, got, keep)
        early_gain, late_gain = early[STATE : STATE + 1], late[STATE : STATE + 1]
        return early[:STATE] + early_gain * late[:STATE], early_gain * late_gain

    tiles = [tile(t) for t in range(5)]
    for b in range(2):
        (one, one_gain), (two, two_gain), (last, last_gain) = tiles[2 * b], tiles[2 * b + 1], tiles[4]
        out_ref[b, :, 0:8, :] = one.reshape(16, 8, 128)
        out_ref[b, :, 8:16, :] = two.reshape(16, 8, 128)
        if b == 1:
            last = pltpu.roll(last, STATE - 4, 0)
        last = jnp.where(upper < 4, last, jnp.where(upper == 4, one_gain, jnp.where(upper == 5, two_gain, last_gain)))
        out_ref[b, :, 16:24, :] = last.reshape(16, 8, 128)


def scan_kernel(in_ref, out_ref):
    rows = iota((8, 128), 0)
    run = [jnp.zeros((8, 128), f32) for _ in range(3)]
    for k in reversed(range(SHARES)):
        tail = in_ref[k, 16:24, :]
        pieces = (in_ref[k, 0:8, :], in_ref[k, 8:16, :], jnp.where(rows < 4, tail, 0.0))
        for i in range(3):
            out_ref[k, 8 * i : 8 * i + 8, :] = run[i]
            run[i] = pieces[i] + tail[4 + i : 5 + i] * run[i]


def return_kernel(core_ref, back_ref, keep_ref, got_ref, mine_ref, send_ref):
    first = core_ref[0] == 0
    upper = iota((STATE, 128), 0) & 7
    for t in range(5):
        cols = slice(128 * t, 128 * t + 128)
        if t < 4:
            entering = back_ref[t // 2, :, 8 * (t % 2) : 8 * (t % 2) + 8, :].reshape(STATE, 128)
        else:
            low = back_ref[0, :, 16:24, :].reshape(STATE, 128)
            high = back_ref[1, :, 16:24, :].reshape(STATE, 128)
            entering = jnp.where(upper < 4, low, pltpu.roll(high, 4, 0))
        late = jnp.where(first, got_ref[:, cols], keep_ref[:, cols])
        passed = late[:STATE] + late[STATE : STATE + 1] * entering
        mine_ref[:, cols] = jnp.where(first, passed, entering)
        send_ref[:, cols] = jnp.where(first, entering, passed)


def local_kernel(
    reset_ref,
    rate_ref,
    step_ref,
    b_ref,
    c_ref,
    x_ref,
    grad_ref,
    state_ref,
    inner_ref,
    factor_ref,
    high_ref,
    low_ref,
    inner_b_ref,
    mate_ref,
    rate_out_ref,
    pad_ref,
    pairs_ref,
):
    reset = reset_ref[0]
    elapsed, log_decay, steps = small_factors(rate_ref, step_ref, pad_ref, True)
    later = iota((SPAN, 128), 0) >= reset
    no_reset = reset >= SPAN
    middle = log_decay[MIDDLE : MIDDLE + 1, :]
    last_log, last_elapsed = log_decay[SPAN - 1 :, :], elapsed[SPAN - 1 :, :]
    centred = log_decay - middle
    up = packed(jnp.exp(centred))
    down = packed(steps * jnp.exp(-centred))
    end = jnp.where(later | no_reset, jnp.exp(last_log - log_decay), 0.0)
    end_steps = packed(steps * end)
    elapsed_parts = packed(elapsed)
    rows = jnp.concatenate(
        [
            jnp.exp(middle),
            jnp.where(no_reset, jnp.exp(last_log), 0.0) * last_elapsed,
            last_elapsed,
            jnp.zeros((5, 128), f32),
        ],
        axis=0,
    )
    rows = packed(rows)
    row, col = iota((SPAN, SPAN), 0), iota((SPAN, SPAN), 1)
    joined = (col >= row) & ((row >= reset) == (col >= reset))
    b, c = b_ref[...], c_ref[...]
    masked = two_parts(jnp.where(joined, dot(b, c, NT), 0.0))
    c_start = jnp.where(later, 0.0, c.astype(f32)).astype(bf16)
    pairs_ref[...] = jnp.zeros_like(pairs_ref)
    rate_out_ref[...] = jnp.zeros_like(rate_out_ref)

    def step(chunk, carry):
        cols = pl.ds(pl.multiple_of(chunk * CHUNK, CHUNK), CHUNK)
        wide = spread(chunk)
        wide_rows = dot(rows, wide, NN)
        x, grad = x_ref[:, cols].astype(f32), grad_ref[:, cols].astype(f32)
        wide_elapsed = dot(elapsed_parts, wide, NN)
        scaled_grad = dot(up, wide, NN) * grad
        grad_parts = two_parts(scaled_grad)
        aged_parts = two_parts(wide_elapsed * scaled_grad)
        wide_down = dot(down, wide, NN)
        scaled_x = wide_down * x
        pairs_ref[...] += dot3(two_parts(scaled_x), grad_parts, NT)
        plain = dot3(masked, grad_parts, NN)
        aged = dot3(masked, aged_parts, NN)
        inner_ref[:, cols] = wide_down * plain
        inside = jnp.sum(scaled_x * (aged - wide_elapsed * plain), axis=0, keepdims=True)
        state = jnp.transpose(state_ref[cols, :])
        start = dot(c_start, aged_parts[0], TN) + dot(c_start, aged_parts[1], TN)
        entry = wide_rows[0:1] * jnp.sum(state * start, axis=0, keepdims=True)
        factor = dot(end_steps, wide, NN)
        factor_ref[:, cols] = factor
        leaving = factor * x
        high, low = two_parts(leaving)
        high_ref[:, cols] = high
        low_ref[:, cols] = low
        left = two_parts(leaving * (wide_rows[2:3] - wide_elapsed))
        mate_ref[:, cols] = dot(b, left[0], TN) + dot(b, left[1], TN) + wide_rows[1:2] * state
        totals = three_parts(jnp.broadcast_to(inside + entry, (8, CHUNK)))
        rate_out_ref[...] += dot(totals[0], wide, NT) + (
            dot(totals[1], wide, NT) + dot(totals[2], wide, NT)
        )
        return carry

    lax.fori_loop(0, STEPS, step, 0)
    pairs = two_parts(jnp.where(joined, pairs_ref[...], 0.0))
    inner_b_ref[...] = dot(pairs[0], c, NN) + dot(pairs[1], c, NN)


def reduce_kernel(
    core_ref, mine_ref, other_ref, high_ref, low_ref, inner_b_ref, mate_ref, rate_ref,
    all_ref, grad_b_ref, rate_out_ref,
):
    core = core_ref[0]
    all_ref[:, pl.ds(pl.multiple_of(core * HALF, HALF), HALF)] = mine_ref[...]
    all_ref[:, pl.ds(pl.multiple_of((1 - core) * HALF, HALF), HALF)] = other_ref[...]
    total = inner_b_ref[...]
    rate = rate_ref[...]
    for chunk in range(STEPS):
        cols = pl.ds(chunk * CHUNK, CHUNK)
        carried = all_ref[:, cols]
        total += dot3((high_ref[:, cols], low_ref[:, cols]), two_parts(carried), NT)
        sums = jnp.sum(carried * mate_ref[:, cols], axis=0, keepdims=True)
        sums = three_parts(jnp.broadcast_to(sums, (8, CHUNK)))
        wide = spread(chunk)
        rate += dot(sums[0], wide, NT) + (dot(sums[1], wide, NT) + dot(sums[2], wide, NT))
    for i in range(4):
        grad_b_ref[i] = total
    for i in range(64):
        rate_out_ref[i] = rate[0:1]


def inputs_kernel(b_ref, all_ref, inner_ref, factor_ref, out_ref):
    b = b_ref[...]
    for chunk in range(STEPS):
        cols = pl.ds(chunk * CHUNK, CHUNK)
        high, low = two_parts(all_ref[:, cols])
        product = dot(b, high, NN) + dot(b, low, NN)
        out_ref[:, cols] = (inner_ref[:, cols] + factor_ref[:, cols] * product).astype(bf16)


SMEM = pl.BlockSpec(memory_space=pltpu.SMEM)
VMEM = pl.BlockSpec(memory_space=pltpu.VMEM)
ANY = pl.BlockSpec(memory_space=pl.ANY)


def call(
    kernel, name, smem, args, outs, scratch=(), flops=1_000_000, size=1_000_000, after=(), grant=8
):
    def run(*refs):
        kernel(*refs[: len(args)], *refs[len(args) + len(after) :])

    return pl.pallas_call(
        run,
        name=name,
        in_specs=[SMEM] * smem + [VMEM] * (len(args) - smem) + [ANY] * len(after),
        out_specs=[VMEM] * len(outs),
        out_shape=[jax.ShapeDtypeStruct(shape, dtype) for shape, dtype in outs],
        scratch_shapes=[pltpu.VMEM(shape, dtype) for shape, dtype in scratch],
        cost_estimate=pl.CostEstimate(flops=flops, bytes_accessed=size, transcendentals=0),
        compiler_params=pltpu.CompilerParams(vmem_limit_bytes=grant << 20),
    )(*args, *after)


def body(inputs, time_step, decay_rate, input_map, output_map, output_grad, span_states, resets):
    core = lax.axis_index(CORE).astype(jnp.int32).reshape(1)
    states = span_states.reshape(COLS, STATE)
    swap = [(0, 1), (1, 0)]
    keep, send = call(
        boundary_kernel, "boundary", 3,
        (resets, core, decay_rate, time_step, output_map, output_grad),
        [((STATE + 8, HALF), f32)] * 2,
        [((128, SPAN), f32), ((STATE + 8, COLS), f32)],
    )
    got = lax.ppermute(send, CORE, swap)
    (pieces,) = call(combine_kernel, "combine", 1, (core, keep, got), [((2, 16, 24, 128), f32)])
    received = lax.all_to_all(pieces.reshape(SHARES, 24, 128), CHIPS, 0, 0, tiled=True)
    inner, factor, high, low, inner_b, mate, rate_local = call(
        local_kernel, "local", 2,
        (resets, decay_rate, time_step, input_map, output_map, inputs, output_grad, states),
        [
            ((SPAN, COLS), f32), ((SPAN, COLS), f32), ((SPAN, COLS), bf16), ((SPAN, COLS), bf16),
            ((SPAN, STATE), f32), ((STATE, COLS), f32), ((8, 128), f32),
        ],
        [((128, SPAN), f32), ((SPAN, SPAN), f32)],
        flops=6_000_000_000, size=8_000_000, after=(pieces,), grant=16,
    )
    (exclusive,) = call(scan_kernel, "carry", 0, (received,), [((SHARES, 24, 128), f32)], after=(rate_local,))
    back = lax.all_to_all(exclusive, CHIPS, 0, 0, tiled=True)
    mine, onward = call(
        return_kernel, "spread", 1, (core, back.reshape(2, 16, 24, 128), keep, got),
        [((STATE, HALF), f32)] * 2,
    )
    other = lax.ppermute(onward, CORE, swap)
    carried, grad_b, rate = call(
        reduce_kernel, "reduce", 1, (core, mine, other, high, low, inner_b, mate, rate_local),
        [((STATE, COLS), f32), ((4, SPAN, STATE), f32), ((64, 1, 128), f32)],
    )
    rates = lax.all_to_all(rate, SEQ, 0, 0, tiled=True)
    grad_bs = lax.all_to_all(grad_b, "head", 0, 0, tiled=True)
    (grad_inputs,) = call(
        inputs_kernel, "inputs", 0, (input_map, carried, inner, factor), [((SPAN, COLS), bf16)],
        flops=2_000_000_000, size=4_000_000,
    )
    grad_rate = -jnp.sum(rates[:, 0, :HEADS], axis=0)
    return grad_inputs, jnp.sum(grad_bs, axis=0), grad_rate


def solution(mesh):
    split = Mesh(
        mesh.devices.reshape(8, 4, 2, mesh.shape["head"]), ("seq_0", "seq_1", "seq_2", "head")
    )
    placed = (
        P(SEQ, "head"),
        P("head", SEQ),
        P("head"),
        P(SEQ, None),
        P(SEQ, None),
        P(SEQ, "head"),
        P(SEQ, "head", None, None),
        P(SEQ),
    )
    return jax.shard_map(
        body,
        mesh=split,
        in_specs=placed,
        out_specs=(P(SEQ, "head"), P(SEQ, None), P("head")),
        check_vma=False,
    )
```

```python
import functools

import jax
import jax.numpy as jnp
from jax import lax
from jax.experimental import pallas as pl
from jax.experimental.pallas import tpu as pltpu
from jax.sharding import Mesh
from jax.sharding import PartitionSpec as P

CHIPS = ("seq_0", "seq_1")
CORE = "seq_2"
SEQ = CHIPS + (CORE,)
f32, bf16 = jnp.float32, jnp.bfloat16

HEADS, WIDTH, STATE, SPAN = 20, 64, 128, 256
COLS = HEADS * WIDTH
HALF = COLS // 2
CHUNK = 256
STEPS = COLS // CHUNK
SHARES = 32
MIDDLE = SPAN // 2 - 1

NN = (((1,), (0,)), ((), ()))
NT = (((1,), (1,)), ((), ()))
TN = (((0,), (0,)), ((), ()))


def dot(a, b, dims):
    return lax.dot_general(a, b, dims, preferred_element_type=f32)


def two_parts(a):
    high = a.astype(bf16)
    return high, (a - high.astype(f32)).astype(bf16)


def three_parts(a):
    high = a.astype(bf16)
    rest = a - high.astype(f32)
    mid = rest.astype(bf16)
    return high, mid, (rest - mid.astype(f32)).astype(bf16)


def dot3(a, b, dims):
    return dot(a[0], b[0], dims) + (dot(a[0], b[1], dims) + dot(a[1], b[0], dims))


def iota(shape, dim):
    return lax.broadcasted_iota(jnp.int32, shape, dim)


def spread(chunk):
    shape = (128, CHUNK)
    lane = iota(shape, 0)
    head = (iota(shape, 1) + chunk * CHUNK) >> 6
    return jnp.where(((lane & 31) == head) & (lane < 96), 1.0, 0.0).astype(bf16)


def packed(a):
    high, mid, low = three_parts(a)
    lane = iota(a.shape, 1)
    return jnp.where(
        lane < 32, high.astype(f32), jnp.where(lane < 64, mid.astype(f32), low.astype(f32))
    ).astype(bf16)


def small_factors(rate_ref, step_ref, pad_ref, with_steps):
    pad_ref[...] = jnp.zeros_like(pad_ref)
    for copy in range(3):
        pad_ref[32 * copy : 32 * copy + HEADS, :] = step_ref[...]
    parts = three_parts(pad_ref[...])
    row, col = iota((SPAN, SPAN), 0), iota((SPAN, SPAN), 1)
    lower = jnp.where(col <= row, 1.0, 0.0).astype(bf16)
    elapsed = dot(lower, parts[0], NT) + (dot(lower, parts[1], NT) + dot(lower, parts[2], NT))
    lane = iota((1, 128), 1) & 31
    rate = jnp.zeros((1, 128), f32)
    for h in range(HEADS):
        rate = jnp.where(lane == h, rate_ref[h], rate)
    log_decay = -rate * elapsed
    if not with_steps:
        return elapsed, log_decay, None
    same = jnp.where(col == row, 1.0, 0.0).astype(bf16)
    steps = (dot(same, parts[0], NT) + dot(same, parts[1], NT)) + dot(same, parts[2], NT)
    return elapsed, log_decay, steps


def column_copies(sources, buffers, sems):
    return [
        [
            pltpu.make_async_copy(
                src.at[:, pl.ds(k * CHUNK, CHUNK)], dst.at[:, pl.ds(k * CHUNK, CHUNK)], sems.at[i, k]
            )
            for i, (src, dst) in enumerate(zip(sources, buffers))
        ]
        for k in range(STEPS)
    ]


def boundary_kernel(
    reset_ref, core_ref, rate_ref, step_hbm, c_hbm, grad_hbm,
    keep_ref, send_ref,
    pad_ref, all_ref, step_ref, c_ref, grad_ref, sems, small_sems,
):
    get_steps = pltpu.make_async_copy(step_hbm, step_ref, small_sems.at[0])
    get_c = pltpu.make_async_copy(c_hbm, c_ref, small_sems.at[1])
    get_grad = column_copies([grad_hbm], [grad_ref], sems)
    get_steps.start()
    for copies in get_grad:
        copies[0].start()
    get_c.start()
    reset, core = reset_ref[0], core_ref[0]
    get_steps.wait()
    elapsed, log_decay, _ = small_factors(rate_ref, step_ref, pad_ref, False)
    later = iota((SPAN, 128), 0) >= reset
    weight = packed(jnp.where(later, 0.0, jnp.exp(log_decay)))
    gain = jnp.where(reset >= SPAN, jnp.exp(log_decay[SPAN - 1 :, :]), 0.0)
    gain = packed(jnp.broadcast_to(gain, (8, 128)))
    get_c.wait()
    for chunk in range(STEPS):
        cols = pl.ds(chunk * CHUNK, CHUNK)
        wide = spread(chunk)
        wide_weight = dot(weight, wide, NN)
        all_ref[STATE:, cols] = dot(gain, wide, NN)
        get_grad[chunk][0].wait()
        high, low = two_parts(wide_weight * grad_ref[:, cols].astype(f32))
        all_ref[:STATE, cols] = dot(c_ref[...], high, TN) + dot(c_ref[...], low, TN)
    keep_ref[...] = all_ref[:, pl.ds(pl.multiple_of(core * HALF, HALF), HALF)]
    send_ref[...] = all_ref[:, pl.ds(pl.multiple_of((1 - core) * HALF, HALF), HALF)]


def combine_kernel(core_ref, keep_ref, got_ref, out_ref, late_ref):
    first = core_ref[0] == 0
    upper = iota((STATE, 128), 0) & 7

    def tile(t):
        cols = slice(128 * t, 128 * t + 128)
        keep, got = keep_ref[:, cols], got_ref[:, cols]
        early, late = jnp.where(first, keep, got), jnp.where(first, got, keep)
        late_ref[:, cols] = late
        early_gain, late_gain = early[STATE : STATE + 1], late[STATE : STATE + 1]
        return early[:STATE] + early_gain * late[:STATE], early_gain * late_gain

    tiles = [tile(t) for t in range(5)]
    for b in range(2):
        (one, one_gain), (two, two_gain), (last, last_gain) = tiles[2 * b], tiles[2 * b + 1], tiles[4]
        out_ref[b, :, 0:8, :] = one.reshape(16, 8, 128)
        out_ref[b, :, 8:16, :] = two.reshape(16, 8, 128)
        if b == 1:
            last = pltpu.roll(last, STATE - 4, 0)
        last = jnp.where(upper < 4, last, jnp.where(upper == 4, one_gain, jnp.where(upper == 5, two_gain, last_gain)))
        out_ref[b, :, 16:24, :] = last.reshape(16, 8, 128)


def scan_kernel(in_ref, out_ref):
    rows = iota((8, 128), 0)
    run = [jnp.zeros((8, 128), f32) for _ in range(3)]
    for k in reversed(range(SHARES)):
        tail = in_ref[k, 16:24, :]
        pieces = (in_ref[k, 0:8, :], in_ref[k, 8:16, :], jnp.where(rows < 4, tail, 0.0))
        for i in range(3):
            out_ref[k, 8 * i : 8 * i + 8, :] = run[i]
            run[i] = pieces[i] + tail[4 + i : 5 + i] * run[i]


def return_kernel(core_ref, back_ref, late_ref, mine_ref, send_ref):
    first = core_ref[0] == 0
    upper = iota((STATE, 128), 0) & 7
    for t in range(5):
        cols = slice(128 * t, 128 * t + 128)
        if t < 4:
            entering = back_ref[t // 2, :, 8 * (t % 2) : 8 * (t % 2) + 8, :].reshape(STATE, 128)
        else:
            low = back_ref[0, :, 16:24, :].reshape(STATE, 128)
            high = back_ref[1, :, 16:24, :].reshape(STATE, 128)
            entering = jnp.where(upper < 4, low, pltpu.roll(high, 4, 0))
        late = late_ref[:, cols]
        passed = late[:STATE] + late[STATE : STATE + 1] * entering
        mine_ref[:, cols] = jnp.where(first, passed, entering)
        send_ref[:, cols] = jnp.where(first, entering, passed)


def local_kernel(
    reset_ref, rate_ref, step_hbm, b_hbm, c_hbm, x_hbm, grad_hbm, state_hbm,
    inner_hbm, end_ref, high_ref, low_ref, inner_b_ref, mate_ref, rate_out_ref,
    pad_ref, pairs_ref, step_ref, b_ref, c_ref, x_ref, grad_ref, state_ref, inner_ref,
    sems, small_sems,
):
    small = [
        pltpu.make_async_copy(src, dst, small_sems.at[i])
        for i, (src, dst) in enumerate(((step_hbm, step_ref), (b_hbm, b_ref), (c_hbm, c_ref)))
    ]

    def loads(chunk):
        cols = pl.ds(pl.multiple_of(chunk * CHUNK, CHUNK), CHUNK)
        return (
            pltpu.make_async_copy(x_hbm.at[:, cols], x_ref.at[:, cols], sems.at[0, chunk]),
            pltpu.make_async_copy(grad_hbm.at[:, cols], grad_ref.at[:, cols], sems.at[1, chunk]),
            pltpu.make_async_copy(state_hbm.at[cols, :], state_ref.at[cols, :], sems.at[2, chunk]),
        )

    def store(chunk):
        cols = pl.ds(pl.multiple_of(chunk * CHUNK, CHUNK), CHUNK)
        return pltpu.make_async_copy(inner_ref.at[:, cols], inner_hbm.at[:, cols], sems.at[3, chunk])

    for copy in small:
        copy.start()
    for chunk in range(STEPS):
        for copy in loads(chunk):
            copy.start()
    for copy in small:
        copy.wait()
    reset = reset_ref[0]
    elapsed, log_decay, steps = small_factors(rate_ref, step_ref, pad_ref, True)
    later = iota((SPAN, 128), 0) >= reset
    no_reset = reset >= SPAN
    middle = log_decay[MIDDLE : MIDDLE + 1, :]
    last_log, last_elapsed = log_decay[SPAN - 1 :, :], elapsed[SPAN - 1 :, :]
    centred = log_decay - middle
    up = packed(jnp.exp(centred))
    down = packed(steps * jnp.exp(-centred))
    end = jnp.where(later | no_reset, jnp.exp(last_log - log_decay), 0.0)
    end_steps = packed(steps * end)
    end_ref[...] = end_steps
    elapsed_parts = packed(elapsed)
    rows = jnp.concatenate(
        [
            jnp.exp(middle),
            jnp.where(no_reset, jnp.exp(last_log), 0.0) * last_elapsed,
            last_elapsed,
            jnp.zeros((5, 128), f32),
        ],
        axis=0,
    )
    rows = packed(rows)
    row, col = iota((SPAN, SPAN), 0), iota((SPAN, SPAN), 1)
    joined = (col >= row) & ((row >= reset) == (col >= reset))
    b, c = b_ref[...], c_ref[...]
    masked = two_parts(jnp.where(joined, dot(b, c, NT), 0.0))
    c_start = jnp.where(later, 0.0, c.astype(f32)).astype(bf16)
    pairs_ref[...] = jnp.zeros_like(pairs_ref)
    rate_out_ref[...] = jnp.zeros_like(rate_out_ref)

    def step(chunk, carry):
        cols = pl.ds(pl.multiple_of(chunk * CHUNK, CHUNK), CHUNK)
        wide = spread(chunk)
        wide_rows = dot(rows, wide, NN)
        for copy in loads(chunk):
            copy.wait()
        x, grad = x_ref[:, cols].astype(f32), grad_ref[:, cols].astype(f32)
        wide_elapsed = dot(elapsed_parts, wide, NN)
        scaled_grad = dot(up, wide, NN) * grad
        grad_parts = two_parts(scaled_grad)
        aged_parts = two_parts(wide_elapsed * scaled_grad)
        wide_down = dot(down, wide, NN)
        scaled_x = wide_down * x
        pairs_ref[...] += dot3(two_parts(scaled_x), grad_parts, NT)
        plain = dot3(masked, grad_parts, NN)
        aged = dot3(masked, aged_parts, NN)
        inner_ref[:, cols] = wide_down * plain
        store(chunk).start()
        inside = jnp.sum(scaled_x * (aged - wide_elapsed * plain), axis=0, keepdims=True)
        state = jnp.transpose(state_ref[cols, :])
        start = dot(c_start, aged_parts[0], TN) + dot(c_start, aged_parts[1], TN)
        entry = wide_rows[0:1] * jnp.sum(state * start, axis=0, keepdims=True)
        factor = dot(end_steps, wide, NN)
        leaving = factor * x
        high, low = two_parts(leaving)
        high_ref[:, cols] = high
        low_ref[:, cols] = low
        left = two_parts(leaving * (wide_rows[2:3] - wide_elapsed))
        mate_ref[:, cols] = dot(b, left[0], TN) + dot(b, left[1], TN) + wide_rows[1:2] * state
        totals = three_parts(jnp.broadcast_to(inside + entry, (8, CHUNK)))
        rate_out_ref[...] += dot(totals[0], wide, NT) + (
            dot(totals[1], wide, NT) + dot(totals[2], wide, NT)
        )
        return carry

    lax.fori_loop(0, STEPS, step, 0)
    pairs = two_parts(jnp.where(joined, pairs_ref[...], 0.0))
    inner_b_ref[...] = dot(pairs[0], c, NN) + dot(pairs[1], c, NN)
    for chunk in range(STEPS):
        store(chunk).wait()


def reduce_kernel(
    core_ref, mine_ref, other_ref, high_ref, low_ref, inner_b_ref, mate_ref, rate_ref,
    all_ref, grad_b_ref, rate_out_ref,
):
    core = core_ref[0]
    all_ref[:, pl.ds(pl.multiple_of(core * HALF, HALF), HALF)] = mine_ref[...]
    all_ref[:, pl.ds(pl.multiple_of((1 - core) * HALF, HALF), HALF)] = other_ref[...]
    total = inner_b_ref[...]
    rate = rate_ref[...]
    for chunk in range(STEPS):
        cols = pl.ds(chunk * CHUNK, CHUNK)
        carried = all_ref[:, cols]
        total += dot3((high_ref[:, cols], low_ref[:, cols]), two_parts(carried), NT)
        sums = jnp.sum(carried * mate_ref[:, cols], axis=0, keepdims=True)
        sums = three_parts(jnp.broadcast_to(sums, (8, CHUNK)))
        wide = spread(chunk)
        rate += dot(sums[0], wide, NT) + (dot(sums[1], wide, NT) + dot(sums[2], wide, NT))
    grad_b_ref[...] = total
    for i in range(64):
        rate_out_ref[i] = rate[0:1]


def inputs_kernel(b_hbm, inner_hbm, all_ref, end_ref, out_ref, b_ref, inner_ref, sems, small_sems):
    get_b = pltpu.make_async_copy(b_hbm, b_ref, small_sems.at[0])
    get_inner = column_copies([inner_hbm], [inner_ref], sems)
    get_b.start()
    for copies in get_inner:
        copies[0].start()
    get_b.wait()
    b, end = b_ref[...], end_ref[...]
    for chunk in range(STEPS):
        cols = pl.ds(chunk * CHUNK, CHUNK)
        high, low = two_parts(all_ref[:, cols])
        product = dot(end, spread(chunk), NN) * (dot(b, high, NN) + dot(b, low, NN))
        get_inner[chunk][0].wait()
        out_ref[:, cols] = (inner_ref[:, cols] + product).astype(bf16)


SMEM = pl.BlockSpec(memory_space=pltpu.SMEM)
VMEM = pl.BlockSpec(memory_space=pltpu.VMEM)
ANY = pl.BlockSpec(memory_space=pl.ANY)
HBM = pl.BlockSpec(memory_space=pltpu.HBM)


def in_hbm(a):
    return pltpu.with_memory_space_constraint(a, pltpu.HBM)


def call(kernel, name, scalars, far, near, outs, scratch=(), flops=1_000_000, after=(), grant=4):
    count = len(scalars) + len(far) + len(near)

    def run(*refs):
        kernel(*refs[:count], *refs[count + len(after) :])

    return pl.pallas_call(
        run,
        name=name,
        in_specs=[SMEM] * len(scalars) + [HBM] * len(far) + [VMEM] * len(near) + [ANY] * len(after),
        out_specs=[HBM if place == "far" else VMEM for _, _, place in outs],
        out_shape=[
            {"far": pltpu.HBM, "stored": pltpu.HBM, "near": pltpu.VMEM}[place](shape, dtype)
            if place
            else jax.ShapeDtypeStruct(shape, dtype)
            for shape, dtype, place in outs
        ],
        scratch_shapes=list(scratch),
        cost_estimate=pl.CostEstimate(flops=flops, bytes_accessed=1_000_000, transcendentals=0),
        compiler_params=pltpu.CompilerParams(vmem_limit_bytes=grant << 20),
    )(*scalars, *map(in_hbm, far), *near, *after)


def body(inputs, time_step, decay_rate, input_map, output_map, output_grad, span_states, resets):
    core = lax.axis_index(CORE).astype(jnp.int32).reshape(1)
    decay_rate = in_hbm(decay_rate)
    states = span_states.reshape(COLS, STATE)
    swap = [(0, 1), (1, 0)]
    dma = pltpu.SemaphoreType.DMA
    steps, maps = pltpu.VMEM((HEADS, SPAN), f32), pltpu.VMEM((SPAN, STATE), bf16)
    wide, wide_f32 = pltpu.VMEM((SPAN, COLS), bf16), pltpu.VMEM((SPAN, COLS), f32)
    padded = pltpu.VMEM((128, SPAN), f32)
    keep, send = call(
        boundary_kernel, "boundary",
        (resets, core, decay_rate), (time_step, output_map, output_grad), (),
        [((STATE + 8, HALF), f32, None)] * 2,
        [padded, pltpu.VMEM((STATE + 8, COLS), f32), steps, maps, wide, dma((1, STEPS)), dma((2,))],
    )
    got = lax.ppermute(send, CORE, swap)
    pieces, late = call(
        combine_kernel, "combine", (core,), (), (keep, got),
        [((2, 16, 24, 128), f32, "near"), ((STATE + 8, HALF), f32, None)],
    )
    received = lax.all_to_all(pieces.reshape(SHARES, 24, 128), CHIPS, 0, 0, tiled=True)
    inner, end, high, low, inner_b, mate, rate_local = call(
        local_kernel, "local",
        (resets, decay_rate),
        (time_step, input_map, output_map, inputs, output_grad, states), (),
        [
            ((SPAN, COLS), f32, "far"), ((SPAN, 128), bf16, "stored"), ((SPAN, COLS), bf16, None),
            ((SPAN, COLS), bf16, None), ((SPAN, STATE), f32, None), ((STATE, COLS), f32, None),
            ((8, 128), f32, None),
        ],
        [
            padded, pltpu.VMEM((SPAN, SPAN), f32), steps, maps, maps, wide, wide,
            pltpu.VMEM((COLS, STATE), f32), wide_f32, dma((4, STEPS)), dma((3,)),
        ],
        flops=6_000_000_000, after=(pieces,), grant=12,
    )
    (exclusive,) = call(
        scan_kernel, "carry", (), (), (received,), [((SHARES, 24, 128), f32, None)],
        after=(rate_local,),
    )
    back = lax.all_to_all(exclusive, CHIPS, 0, 0, tiled=True)
    mine, onward = call(
        return_kernel, "spread", (core,), (), (back.reshape(2, 16, 24, 128), late),
        [((STATE, HALF), f32, None)] * 2,
    )
    other = lax.ppermute(onward, CORE, swap)
    carried, grad_b, rate = call(
        reduce_kernel, "reduce", (core,), (), (mine, other, high, low, inner_b, mate, rate_local),
        [((STATE, COLS), f32, None), ((SPAN, STATE), f32, None), ((64, 1, 128), f32, "near")],
    )
    rates = lax.all_to_all(rate, SEQ, 0, 0, tiled=True)
    near, far, across = (
        lax.ppermute(grad_b, "head", [(i, (i + d) % 4) for i in range(4)]) for d in (1, 3, 2)
    )
    (grad_inputs,) = call(
        inputs_kernel, "inputs", (), (input_map, inner), (carried, in_hbm(end)),
        [((SPAN, COLS), bf16, None)],
        [maps, wide_f32, dma((1, STEPS)), dma((1,))], flops=2_000_000_000,
    )
    grad_rate = -jnp.sum(rates[:, 0, :HEADS], axis=0)
    return grad_inputs, (grad_b + across) + (near + far), grad_rate


def solution(mesh):
    split = Mesh(
        mesh.devices.reshape(8, 4, 2, mesh.shape["head"]), ("seq_0", "seq_1", "seq_2", "head")
    )
    placed = (
        P(SEQ, "head"),
        P("head", SEQ),
        P("head"),
        P(SEQ, None),
        P(SEQ, None),
        P(SEQ, "head"),
        P(SEQ, "head", None, None),
        P(SEQ),
    )
    return jax.shard_map(
        body,
        mesh=split,
        in_specs=placed,
        out_specs=(P(SEQ, "head"), P(SEQ, None), P("head")),
        check_vma=False,
    )
```
